32 devices in a mesh: seqa: 4 (over z), seqb: 2 (over x), dp: 4 (over y, core).
Axes of the slice: x: 2, y: 2, z: 4, core: 2. Of those that a mesh axis runs over, the one named last changes fastest.
Arguments:
- queries: bfloat16 [1024, 8, 64], P(('dp', 'seqa', 'seqb')), parts along dimension 0, may hold values from -6 to 6
- keys: bfloat16 [1024, 8, 64], P(('dp', 'seqa', 'seqb')), parts along dimension 0, may hold values from -6 to 6
- values: bfloat16 [1024, 8, 64], P(('dp', 'seqa', 'seqb')), parts along dimension 0, may hold values from -6 to 6
- doc_bounds: int32 [36], P('dp'), parts along dimension 0, may hold values from 0 to 256, as said below
- q_gain: float32 [64], replicated, may hold values from 0.25 to 1.75
- k_gain: float32 [64], replicated, may hold values from 0.25 to 1.75
Outputs:
- attended: bfloat16 [1024, 8, 64], P(('dp', 'seqa', 'seqb')), parts along dimension 0
The draws below stay inside these ranges and needn't reach their ends.
There are 4 independent parts, one for each index of `dp`. The reference program is written for one: setup_inputs(seed, part) draws one part's arguments, and reference() takes and returns one part's arrays. A program takes and returns all parts, laid end to end along the dimension named above; an argument that names none is the same for every part. Nothing has to cross between parts.
Inputs may be any that keep to these rules, and one draw needn't show every extreme that they name: doc_bounds[0] is 0, doc_bounds[8] is 256, and the entries rise strictly.
All inputs are finite; a program needn't handle non-finite values.
Results may differ from the reference program's by a relative error of at most 0.0015.
Values may be sent and summed in bfloat16 or wider, within the bound.
A program may use at most 64 MiB of HBM per device.

```python
import jax
import jax.numpy as jnp
from jax import lax

HD = 64
DOCS = 8
SEQ = 256
HEADS = 8


def draw_doc_bounds(key, part):
    shuffled = jax.random.permutation(key, SEQ - 1).astype(jnp.int32) + 1
    cuts = jnp.sort(shuffled[:DOCS - 1])
    return jnp.concatenate([jnp.zeros((1,), jnp.int32), cuts, jnp.full((1,), SEQ, jnp.int32)]).astype(jnp.int32)


def level_of(stream_key, shape, cuts, least, top_value):
    def one(dim, parts):
        heights = jax.random.uniform(jax.random.fold_in(jax.random.fold_in(stream_key, 6), dim), (parts,), jnp.float32, least / len(cuts), top_value / len(cuts))
        return jnp.repeat(jnp.exp(heights), shape[dim] // parts).reshape((-1,) + (1,) * (len(shape) - dim - 1))

    level = one(*cuts[0])
    for cut in cuts[1:]:
        level = level * one(*cut)
    return level


def normal_values(stream_key, dims, scale, bound, shards=(), kind=jnp.bfloat16):
    values = scale * jax.random.normal(stream_key, dims, jnp.float32)
    if shards:
        values = values * level_of(stream_key, dims, shards, -0.22, 0.18)
    return jnp.clip(values, -bound, bound).astype(kind)


def setup_inputs(seed: int = 0, part: int = 0) -> dict:
    streams_of = jax.random.split(jax.random.key(seed), 7)
    part_keys = jax.random.split(jax.random.fold_in(streams_of[6], part), 7)
    queries = normal_values(part_keys[0], (SEQ, HEADS, HD), 1.0, 6.0, ((0, 8),))
    keys = normal_values(part_keys[1], (SEQ, HEADS, HD), 1.0, 6.0, ((0, 8),))
    values = normal_values(part_keys[2], (SEQ, HEADS, HD), 1.0, 6.0, ((0, 8),))
    doc_bounds = draw_doc_bounds(jax.random.fold_in(jax.random.fold_in(streams_of[6], part), 71), part)
    q_gain = jnp.clip(1.0 + 0.15 * jax.random.normal(streams_of[4], (HD,), jnp.float32), 0.25, 1.75)
    k_gain = jnp.clip(1.0 + 0.15 * jax.random.normal(streams_of[5], (HD,), jnp.float32), 0.25, 1.75)
    return {"queries": queries, "keys": keys, "values": values, "doc_bounds": doc_bounds, "q_gain": q_gain, "k_gain": k_gain}


def prepare(block, gain, positions):
    values32 = block.astype(jnp.float32)
    scale = lax.rsqrt(lax.optimization_barrier(jnp.mean(values32 * values32, axis=-1, keepdims=True)) + 1e-06)
    normed = values32 * scale * gain
    half = normed.shape[-1] // 2
    freq = jnp.exp(-jnp.log(10000.0) * jnp.arange(half, dtype=jnp.float32) * 2.0 / normed.shape[-1])
    angle = positions.astype(jnp.float32)[:, None] * freq[None, :]
    first = normed[:, :half]
    second = normed[:, half:]
    cosine = jnp.cos(angle)
    sine = jnp.sin(angle)
    rotated = jnp.concatenate([first * cosine - second * sine, first * sine + second * cosine], axis=-1)
    return rotated.astype(jnp.bfloat16)

def reference(queries, keys, values, doc_bounds, q_gain, k_gain):
    length = queries.shape[0]
    width = queries.shape[2]
    places = jnp.arange(length, dtype=jnp.int32)
    doc = lax.optimization_barrier(jnp.sum((places[:, None] >= doc_bounds[None, 1:DOCS]).astype(jnp.int32), axis=1)).astype(jnp.int32)
    positions = places - doc_bounds[doc]
    allowed = (doc[:, None] == doc[None, :]) & (places[None, :] <= places[:, None])

    def one_head(items):
        query_head, key_head, value_head = items
        qr = prepare(query_head, q_gain, positions)
        kr = prepare(key_head, k_gain, positions)
        scores = jnp.dot(qr, kr.T, preferred_element_type=jnp.float32) / jnp.sqrt(jnp.float32(width))
        scores = jnp.where(allowed, scores, jnp.float32(-1e+30))
        top = lax.optimization_barrier(jnp.max(scores, axis=1, keepdims=True))
        expo = jnp.where(allowed, jnp.exp(scores - top), jnp.float32(0.0))
        weights = (expo / lax.optimization_barrier(jnp.sum(expo, axis=1, keepdims=True))).astype(jnp.bfloat16)
        return jnp.dot(weights, value_head, preferred_element_type=jnp.float32).astype(jnp.bfloat16)
    outputs = lax.map(one_head, (jnp.transpose(queries, (1, 0, 2)), jnp.transpose(keys, (1, 0, 2)), jnp.transpose(values, (1, 0, 2))))
    return jnp.transpose(outputs, (1, 0, 2))
```

```python
import functools

import jax
import jax.numpy as jnp
from jax import lax
from jax.experimental import pallas as pl
from jax.experimental.pallas import tpu as pltpu
from jax.sharding import PartitionSpec as P

MESH = pl.DeviceIdType.MESH
TOK_DEV = 32
DOCS = 8


def cos_sin(angle):
    turns = jnp.floor(angle * 0.6366197723675814 + 0.5)
    r = angle - turns * 1.5703125
    r = r - turns * 4.837512969970703125e-4
    r = r - turns * 7.54978995489188216e-8
    z = r * r
    s = ((-1.9515295891e-4 * z + 8.3321608736e-3) * z - 1.6666654611e-1) * z * r + r
    c = ((2.443315711809948e-5 * z - 1.388731625493765e-3) * z + 4.166664568298827e-2) * z * z
    c = c - 0.5 * z + 1.0
    quarter = turns.astype(jnp.int32)
    odd = (quarter & 1) == 1
    cosine = jnp.where(odd, s, c)
    sine = jnp.where(odd, c, s)
    cosine = jnp.where(((quarter + 1) & 2) == 2, -cosine, cosine)
    sine = jnp.where((quarter & 2) == 2, -sine, sine)
    return cosine, sine


def starts_of(places, doc):
    start = jnp.zeros_like(places)
    for d in range(1, doc.shape[0] - 1):
        start = jnp.where(places >= doc[d], doc[d], start)
    return start


def kernel(
    nb, q_hbm, k_hbm, v_hbm, doc_hbm, qg_hbm, kg_hbm, out_ref,
    qb, kb, vb, doc, qg, kg, rows_qk, rows_v, send, recv, back, gathered, rows_out,
    in_sem, send_sem, recv_sem, back_send, back_recv,
):
    tok, heads, width = qb.shape
    n = recv.shape[0]
    half, pair = tok // 2, 2 * width
    me = lax.axis_index("seqa") * nb + lax.axis_index("seqb")

    def place(m):
        peer = lax.rem(me + m, n)
        return peer, {"seqa": peer // nb, "seqb": lax.rem(peer, nb)}

    barrier = pltpu.get_barrier_semaphore()
    for m in range(1, n):
        pl.semaphore_signal(barrier, inc=1, device_id=place(m)[1], device_id_type=MESH)
    loads = [
        pltpu.make_async_copy(src, dst, in_sem.at[i])
        for i, (src, dst) in enumerate(
            ((doc_hbm, doc), (qg_hbm, qg), (kg_hbm, kg), (q_hbm, qb), (k_hbm, kb), (v_hbm, vb))
        )
    ]
    for load in loads:
        load.start()
    for load in loads[:3]:
        load.wait()

    lane = lax.broadcasted_iota(jnp.int32, (tok, pair), 1)
    low = lane < width
    places = me * tok + lax.broadcasted_iota(jnp.int32, (tok, pair), 0)
    within = lax.rem(lane, width // 2).astype(jnp.float32)
    freq = jnp.exp(within * (-2.0 / width * 9.210340371976184))
    cosine, sine = cos_sin((places - starts_of(places, doc)).astype(jnp.float32) * freq)
    first = lax.rem(lane, width) < width // 2
    sine = jnp.where(first, -sine, sine)
    gain = jnp.concatenate([qg[...] * width**-0.5, kg[...]], axis=-1)

    for load in loads[3:]:
        load.wait()
    rows_qk[:, :width] = qb[...].astype(jnp.float32).reshape(tok * heads, width)
    rows_qk[:, width:] = kb[...].astype(jnp.float32).reshape(tok * heads, width)
    rows_v[...] = vb[...].astype(jnp.float32).reshape(tok * heads, width)
    for h in range(heads):
        x = rows_qk[pl.ds(h, tok, stride=heads), :]
        v = rows_v[pl.ds(h, tok, stride=heads), :]
        square = x * x
        total_q = jnp.sum(jnp.where(low, square, 0.0), axis=-1, keepdims=True)
        total_k = jnp.sum(jnp.where(low, 0.0, square), axis=-1, keepdims=True)
        x = x * lax.rsqrt(jnp.where(low, total_q, total_k) / width + 1e-06) * gain
        other = jnp.where(
            first, pltpu.roll(x, pair - width // 2, 1), pltpu.roll(x, width // 2, 1)
        )
        x = x * cosine + other * sine
        kv = jnp.concatenate([x[:, width:], v], axis=-1)
        qq = jnp.concatenate([x[:half, :width], x[half:, :width]], axis=-1)
        send[h, :tok, :] = kv.astype(jnp.bfloat16)
        send[h, tok:, :] = qq.astype(jnp.bfloat16)
    recv[me] = send[me]

    q_places = [
        lax.broadcasted_iota(jnp.int32, (n, half, 1), 0) * tok
        + lax.broadcasted_iota(jnp.int32, (n, half, 1), 1)
        + part * half
        for part in range(2)
    ]
    q_places = [x.reshape(n * half, 1) for x in q_places]
    q_starts = [starts_of(x, doc) for x in q_places]

    pl.semaphore_wait(barrier, n - 1)

    def exchange(source, target, sems, m):
        peer, coords = place(m)
        return pltpu.make_async_remote_copy(
            src_ref=source.at[peer],
            dst_ref=target.at[me],
            send_sem=sems[0].at[m - 1],
            recv_sem=sems[1].at[m - 1],
            device_id=coords,
            device_id_type=MESH,
        )

    out = [exchange(send, recv, (send_sem, recv_sem), m) for m in range(1, n)]
    for copy in out:
        copy.start()
    for copy in out:
        copy.wait_recv()

    outs = []
    for part in range(2):
        kv = recv[:, :tok, :].reshape(n * tok, pair)
        q = recv[:, tok:, part * width : (part + 1) * width].reshape(n * half, width)
        scores = lax.dot_general(
            q, kv[:, :width], (((1,), (1,)), ((), ())), preferred_element_type=jnp.float32
        )
        key = lax.broadcasted_iota(jnp.int32, scores.shape, 1)
        allowed = (key >= q_starts[part]) & (key <= q_places[part])
        expo = jnp.where(allowed, jnp.exp(scores), 0.0)
        weights = (expo * (1.0 / jnp.sum(expo, axis=1, keepdims=True))).astype(jnp.bfloat16)
        both = jnp.dot(weights, kv, preferred_element_type=jnp.float32)
        outs.append(both[:, width:])
    back[...] = (
        jnp.concatenate(outs, axis=-1).astype(jnp.bfloat16).reshape(n, half, pair)
    )
    home = [exchange(back, gathered, (back_send, back_recv), m) for m in range(1, n)]
    for copy in home:
        copy.start()
    gathered[me] = back[me]
    for copy in out:
        copy.wait_send()
    for copy in home:
        copy.wait_recv()
    for h in range(heads):
        block = gathered[h].astype(jnp.float32)
        rows_out[pl.ds(h, half, stride=heads), :] = block[:, :width]
        rows_out[pl.ds(half * heads + h, half, stride=heads), :] = block[:, width:]
    out_ref[...] = rows_out[...].reshape(tok, heads, width).astype(jnp.bfloat16)
    for copy in home:
        copy.wait_send()


def fused(n, nb, queries, keys, values, doc_bounds, q_gain, k_gain):
    tok, heads, width = queries.shape
    half, pair = tok // 2, 2 * width
    block = pltpu.VMEM((tok, heads, width), jnp.bfloat16)
    dma = pltpu.SemaphoreType.DMA((n - 1,))
    return pl.pallas_call(
        functools.partial(kernel, nb),
        out_shape=jax.ShapeDtypeStruct(queries.shape, queries.dtype),
        in_specs=[pl.BlockSpec(memory_space=pl.ANY)] * 6,
        out_specs=pl.BlockSpec(memory_space=pltpu.VMEM),
        scratch_shapes=[
            block, block, block,
            pltpu.SMEM(doc_bounds.shape, jnp.int32),
            pltpu.VMEM((1, width), jnp.float32),
            pltpu.VMEM((1, width), jnp.float32),
            pltpu.VMEM((tok * heads, pair), jnp.float32),
            pltpu.VMEM((tok * heads, width), jnp.float32),
            pltpu.VMEM((n, tok + half, pair), jnp.bfloat16),
            pltpu.VMEM((n, tok + half, pair), jnp.bfloat16),
            pltpu.VMEM((n, half, pair), jnp.bfloat16),
            pltpu.VMEM((n, half, pair), jnp.bfloat16),
            pltpu.VMEM((tok * heads, width), jnp.float32),
            pltpu.SemaphoreType.DMA((6,)),
            dma, dma, dma, dma,
        ],
        compiler_params=pltpu.CompilerParams(collective_id=0, has_side_effects=True),
    )(queries, keys, values, doc_bounds, q_gain.reshape(1, width), k_gain.reshape(1, width))


def for_sending(value):
    return jax.tree.map(lambda a: a.astype(jnp.bfloat16) if a.dtype == jnp.float32 else a, value)


def prepare(block, gain, positions):
    values32 = block.astype(jnp.float32)
    scale = lax.rsqrt(jnp.mean(values32 * values32, axis=-1, keepdims=True) + 1e-06)
    normed = values32 * scale * gain
    half = normed.shape[-1] // 2
    freq = jnp.exp(-jnp.log(10000.0) * jnp.arange(half, dtype=jnp.float32) * 2.0 / normed.shape[-1])
    angle = positions.astype(jnp.float32)[:, None] * freq[None, :]
    first = normed[:, :half]
    second = normed[:, half:]
    cosine = jnp.cos(angle)
    sine = jnp.sin(angle)
    rotated = jnp.concatenate(
        [first * cosine - second * sine, first * sine + second * cosine], axis=-1
    )
    return rotated.astype(jnp.bfloat16)


def attend_head(query_head, key_head, value_head, doc_bounds, q_gain, k_gain):
    length, width = query_head.shape
    places = jnp.arange(length, dtype=jnp.int32)
    doc = jnp.sum((places[:, None] >= doc_bounds[None, 1:DOCS]).astype(jnp.int32), axis=1).astype(
        jnp.int32
    )
    positions = places - doc_bounds[doc]
    qr = prepare(query_head, q_gain, positions)
    kr = prepare(key_head, k_gain, positions)
    block = 8 * TOK_DEV
    count = length // block

    def one_block(items):
        query_rows, query_doc, query_place = items
        scores = jnp.dot(query_rows, kr.T, preferred_element_type=jnp.float32) / jnp.sqrt(
            jnp.float32(width)
        )
        allowed = (query_doc[:, None] == doc[None, :]) & (places[None, :] <= query_place[:, None])
        scores = jnp.where(allowed, scores, jnp.float32(-1e30))
        top = jnp.max(scores, axis=1, keepdims=True)
        expo = jnp.where(allowed, jnp.exp(scores - top), jnp.float32(0.0))
        weights = (expo / jnp.sum(expo, axis=1, keepdims=True)).astype(jnp.bfloat16)
        return jnp.dot(weights, value_head, preferred_element_type=jnp.float32).astype(jnp.bfloat16)

    outputs = lax.map(
        one_block,
        (qr.reshape(count, block, width), doc.reshape(count, block), places.reshape(count, block)),
    )
    return outputs.reshape(length, width)


def body(queries, keys, values, doc_bounds, q_gain, k_gain):
    query_full, key_full, value_full = (
        lax.all_to_all(queries, ("seqa", "seqb"), split_axis=1, concat_axis=0, tiled=True),
        lax.all_to_all(keys, ("seqa", "seqb"), split_axis=1, concat_axis=0, tiled=True),
        lax.all_to_all(values, ("seqa", "seqb"), split_axis=1, concat_axis=0, tiled=True),
    )
    attend_all = jax.vmap(attend_head, in_axes=(1, 1, 1, None, None, None), out_axes=1)
    result = attend_all(query_full, key_full, value_full, doc_bounds, q_gain, k_gain)
    back = jax.tree.map(
        lambda part, own: part.astype(own.dtype),
        lax.all_to_all(
            for_sending(result), ("seqa", "seqb"), split_axis=0, concat_axis=1, tiled=True
        ),
        result,
    )
    return back


def solution(mesh):
    placed = (
        P(("dp", "seqa", "seqb"), None, None),
        P(("dp", "seqa", "seqb"), None, None),
        P(("dp", "seqa", "seqb"), None, None),
        P("dp"),
        P(),
        P(),
    )
    nb = mesh.shape["seqb"]
    n = mesh.shape["seqa"] * nb

    def local(queries, keys, values, doc_bounds, q_gain, k_gain):
        tok, heads, width = queries.shape
        fits = heads == n and heads == 8 and tok % 32 == 0 and n * tok <= 512 and width == 64
        step = functools.partial(fused, n, nb) if fits else body
        return step(queries, keys, values, doc_bounds, q_gain, k_gain)

    return jax.shard_map(
        local,
        mesh=mesh,
        in_specs=placed,
        out_specs=P(("dp", "seqa", "seqb"), None, None),
        check_vma=False,
    )
```
